32 devices in a mesh: branch: 2 (over core), dp: 4 (over y, x), mp: 4 (over z).
Axes of the slice: x: 2, y: 2, z: 4, core: 2. Of those that a mesh axis runs over, the one named last changes fastest.
Arguments:
- unet_hidden: bfloat16 [8, 1280, 256], P(('branch', 'dp'), 'mp'), may hold values from -6 to 6
- control_hidden: bfloat16 [2, 2, 4, 1280, 256], P('branch', None, 'dp', 'mp'), may hold values from -6 to 6
- timesteps: int32 [2, 4], P(None, 'dp'), may hold values from 0 to 999
- control_scales: int32 [2, 2, 4], P('branch', None, 'dp'), may hold values from 1 to 16
- unet_time_first: bfloat16 [320, 1280], replicated, may hold values from -0.3125 to 0.3125
- unet_time_second: bfloat16 [1280, 1280], replicated, may hold values from -0.15625 to 0.15625
- unet_proj: bfloat16 [1280, 1280], P(None, 'mp'), may hold values from -0.15625 to 0.15625
- unet_conv_first: bfloat16 [9, 1280, 1280], P(None, 'mp'), may hold values from -0.0546875 to 0.0546875
- unet_conv_second: bfloat16 [9, 1280, 1280], P(None, 'mp'), may hold values from -0.0546875 to 0.0546875
- control_time_first: bfloat16 [2, 320, 1280], P('branch'), may hold values from -0.3125 to 0.3125
- control_time_second: bfloat16 [2, 1280, 1280], P('branch'), may hold values from -0.15625 to 0.15625
- control_proj: bfloat16 [2, 1280, 1280], P('branch', None, 'mp'), may hold values from -0.15625 to 0.15625
- control_conv_first: bfloat16 [2, 9, 1280, 1280], P('branch', None, 'mp'), may hold values from -0.0546875 to 0.0546875
- control_conv_second: bfloat16 [2, 9, 1280, 1280], P('branch', None, 'mp'), may hold values from -0.0546875 to 0.0546875
- zero_conv: bfloat16 [2, 1280, 1280], P('branch', 'mp'), may hold values from -0.15625 to 0.15625
Outputs:
- skip_out: bfloat16 [8, 1280, 256], P(('branch', 'dp'), 'mp')
The draws below stay inside these ranges and needn't reach their ends.
All inputs are finite; a program needn't handle non-finite values.
Results may differ from the reference program's by a relative error of at most 0.018.
Values may be sent and summed in bfloat16 or wider, within the bound.
A program may use at most 128 MiB of HBM per device.

```python
import math
import jax
import jax.numpy as jnp
from jax import lax

C = 1280
TDIM = 320
GROUPS = 32
SIDE = 16
COPIES = 2
HW = 256
HALVES = 2
BATCH = 8


def plant(entries, key, smallest, high):
    index_at = [jax.random.randint(jax.random.fold_in(key, axis), (), 0, length) for axis, length in enumerate(entries.shape)]
    main_axis = entries.shape.index(max(entries.shape))
    beside = index_at[:main_axis] + [(index_at[main_axis] + 1) % entries.shape[main_axis]] + index_at[main_axis + 1:]
    return entries.at[tuple(index_at)].set(smallest).at[tuple(beside)].set(high)


def shard_levels(rng, extent, split, smallest, top_value):
    factor_of, own = 1.0, jax.random.fold_in(rng, 6)
    for dim, parts in split:
        heights = jnp.exp(jax.random.uniform(jax.random.fold_in(own, dim), (parts,), jnp.float32, smallest / len(split), top_value / len(split)))
        factor_of = factor_of * jnp.repeat(heights, extent[dim] // parts).reshape([-1 if axis == dim else 1 for axis in range(len(extent))])
    return factor_of


def centred(stream_key, extent, deviation, most, cuts=(), held_as=jnp.bfloat16):
    level = shard_levels(stream_key, extent, cuts, -0.22, 0.18) if cuts else 1.0
    array = jax.random.normal(stream_key, extent, jnp.float32) * deviation * level
    return jnp.minimum(jnp.maximum(array, -most), most).astype(held_as)


def setup_inputs(seed: int = 0) -> dict:
    key_list = jax.random.split(jax.random.key(seed), 16)
    unet_hidden = centred(key_list[0], (BATCH, C, HW), 1.0, 6.0, ((0, 8), (1, 4)))
    control_hidden = centred(key_list[1], (COPIES, HALVES, BATCH // HALVES, C, HW), 1.0, 6.0, ((0, 2), (2, 4), (3, 4)))
    timesteps = plant(jax.random.randint(key_list[2], (HALVES, BATCH // HALVES), 0, 1000), jax.random.fold_in(key_list[2], 1), 0, 999).astype(jnp.int32)
    control_scales = plant(jax.random.randint(key_list[3], (COPIES, HALVES, BATCH // HALVES), 1, 17), jax.random.fold_in(key_list[3], 1), 1, 16).astype(jnp.int32)
    unet_time_first = centred(key_list[4], (TDIM, C), TDIM ** -0.5, 0.3125)
    unet_time_second = centred(key_list[5], (C, C), C ** -0.5, 0.15625)
    unet_proj = centred(key_list[6], (C, C), C ** -0.5, 0.15625, ((1, 4),))
    unet_conv_first = centred(key_list[7], (9, C, C), (9 * C) ** -0.5, 0.0546875, ((1, 4),))
    unet_conv_second = centred(key_list[8], (9, C, C), (9 * C) ** -0.5, 0.0546875, ((1, 4),))
    control_time_first = centred(key_list[9], (COPIES, TDIM, C), TDIM ** -0.5, 0.3125, ((0, 2),))
    control_time_second = centred(key_list[10], (COPIES, C, C), C ** -0.5, 0.15625, ((0, 2),))
    control_proj = centred(key_list[11], (COPIES, C, C), C ** -0.5, 0.15625, ((0, 2), (2, 4)))
    control_conv_first = centred(key_list[12], (COPIES, 9, C, C), (9 * C) ** -0.5, 0.0546875, ((0, 2), (2, 4)))
    control_conv_second = centred(key_list[13], (COPIES, 9, C, C), (9 * C) ** -0.5, 0.0546875, ((0, 2), (2, 4)))
    zero_conv = centred(key_list[14], (COPIES, C, C), C ** -0.5, 0.15625, ((0, 2), (1, 4)))
    return dict(unet_hidden=unet_hidden, control_hidden=control_hidden, timesteps=timesteps, control_scales=control_scales, unet_time_first=unet_time_first, unet_time_second=unet_time_second, unet_proj=unet_proj, unet_conv_first=unet_conv_first, unet_conv_second=unet_conv_second, control_time_first=control_time_first, control_time_second=control_time_second, control_proj=control_proj, control_conv_first=control_conv_first, control_conv_second=control_conv_second, zero_conv=zero_conv)


def sinusoid(step_ids):
    half_width = TDIM // 2
    frequency = jnp.exp(-math.log(10000.0) * jnp.arange(half_width, dtype=jnp.float32) / half_width)
    angles = step_ids.astype(jnp.float32)[:, None] * frequency[None, :]
    return jnp.concatenate([jnp.cos(angles), jnp.sin(angles)], axis=1)

def time_embed(step_ids, first_weight, second_weight):
    waves = sinusoid(step_ids).astype(jnp.bfloat16)
    middle = jax.nn.silu(jnp.dot(waves, first_weight, preferred_element_type=jnp.float32)).astype(jnp.bfloat16)
    embedded = jnp.dot(middle, second_weight, preferred_element_type=jnp.float32)
    return jax.nn.silu(embedded).astype(jnp.bfloat16)

def norm_silu(values):
    image_count, width, pixels = values.shape
    group_size = C // GROUPS
    grouped = values.reshape(image_count, width // group_size, group_size, pixels)
    group_mean = lax.optimization_barrier(jnp.mean(grouped, axis=(2, 3), keepdims=True))
    centered = grouped - group_mean
    group_var = lax.optimization_barrier(jnp.mean(centered * centered, axis=(2, 3), keepdims=True))
    normed = centered * lax.rsqrt(group_var + 1e-05)
    return jax.nn.silu(normed).reshape(image_count, width, pixels)

def conv_taps(activation, weight, einsum_form):
    image_count, width, pixels = activation.shape
    image_grid = activation.astype(jnp.float32).reshape(image_count, width, SIDE, SIDE)
    padded = jnp.pad(image_grid, ((0, 0), (0, 0), (1, 1), (1, 1)))
    accum_sum = None
    for tap_index in range(9):
        row_shift = tap_index // 3
        col_shift = tap_index % 3
        window = padded[:, :, row_shift:row_shift + SIDE, col_shift:col_shift + SIDE].reshape(image_count, width, pixels)
        term = jnp.einsum(einsum_form, weight[tap_index].astype(jnp.float32), window, precision=lax.Precision.HIGHEST)
        accum_sum = term if accum_sum is None else accum_sum + term
    return accum_sum

def resnet_block(hidden, conv_first, conv_second, time_proj, time_act):
    first_act = norm_silu(hidden.astype(jnp.float32)).astype(jnp.bfloat16)
    inner_sum = conv_taps(first_act, conv_first, 'oc,bcp->bop')
    inner_sum = inner_sum + jnp.dot(time_act, time_proj, preferred_element_type=jnp.float32)[:, :, None]
    second_act = norm_silu(inner_sum).astype(jnp.bfloat16)
    return hidden.astype(jnp.float32) + conv_taps(second_act, conv_second, 'co,bcp->bop')

def reference(unet_hidden, control_hidden, timesteps, control_scales, unet_time_first, unet_time_second, unet_proj, unet_conv_first, unet_conv_second, control_time_first, control_time_second, control_proj, control_conv_first, control_conv_second, zero_conv):
    step_ids = timesteps.reshape(BATCH)
    unet_act = time_embed(step_ids, unet_time_first, unet_time_second)
    unet_out = resnet_block(unet_hidden, unet_conv_first, unet_conv_second, unet_proj, unet_act)
    residual = jnp.zeros((BATCH, C, HW), jnp.float32)
    for copy_index in range(COPIES):
        copy_act = time_embed(step_ids, control_time_first[copy_index], control_time_second[copy_index])
        copy_hidden = control_hidden[copy_index].reshape(BATCH, C, HW)
        copy_out = resnet_block(copy_hidden, control_conv_first[copy_index], control_conv_second[copy_index], control_proj[copy_index], copy_act).astype(jnp.bfloat16)
        scale_factor = control_scales[copy_index].reshape(BATCH).astype(jnp.float32) / 8.0
        zero_terms = jnp.einsum('co,bcp->bop', zero_conv[copy_index].astype(jnp.float32), copy_out.astype(jnp.float32), precision=lax.Precision.HIGHEST)
        residual = residual + scale_factor[:, None, None] * zero_terms
    return (unet_out + residual).astype(jnp.bfloat16)
```

```python
import functools
import math

import jax
import jax.numpy as jnp
from jax import lax
from jax.experimental import pallas as pl
from jax.experimental.pallas import tpu as pltpu
from jax.sharding import PartitionSpec as P

TDIM = 320
GROUP = 40
SIDE = 16
MESH = pl.DeviceIdType.MESH


def sinusoid(step_ids):
    half_width = TDIM // 2
    frequency = jnp.exp(-math.log(10000.0) * jnp.arange(half_width, dtype=jnp.float32) / half_width)
    angles = step_ids.astype(jnp.float32)[:, None] * frequency[None, :]
    return jnp.concatenate([jnp.cos(angles), jnp.sin(angles)], axis=1)


def time_embed(waves, first_weight, second_weight):
    middle = jax.nn.silu(jnp.dot(waves, first_weight, preferred_element_type=jnp.float32)).astype(
        jnp.bfloat16
    )
    embedded = jnp.dot(middle, second_weight, preferred_element_type=jnp.float32)
    return jax.nn.silu(embedded).astype(jnp.bfloat16)


def norm_silu(values):
    width, pixels = values.shape
    grouped = values.reshape(width // GROUP, GROUP, pixels)
    count = 1.0 / (GROUP * pixels)
    mean = jnp.sum(jnp.sum(grouped, axis=1, keepdims=True), axis=2, keepdims=True) * count
    centered = grouped - mean
    var = jnp.sum(jnp.sum(centered * centered, axis=1, keepdims=True), axis=2, keepdims=True) * count
    normed = centered * lax.rsqrt(var + 1e-05)
    return jax.nn.silu(normed).reshape(width, pixels)


def kernel(
    ways,
    unet_hidden,
    control_hidden,
    start,
    scale,
    first_u,
    second_u,
    first_c,
    second_c,
    zero,
    out,
    w1u,
    w2u,
    w1c,
    w2c,
    wz,
    gathered,
    inner,
    flipped,
    total_c,
    total_u,
    sends,
    lands,
    swap_out,
    swap_in,
    load_sem,
    ag_send,
    ag_recv,
    rs_send,
    rs_recv,
    swap_send,
    swap_recv,
):
    branch = lax.axis_index("branch")
    dp = lax.axis_index("dp")
    me = lax.axis_index("mp")
    width, pixels = unet_hidden.shape[1], unet_hidden.shape[2]
    channels = ways * width

    loads = [
        pltpu.make_async_copy(src, dst, load_sem.at[i])
        for i, (src, dst) in enumerate(
            ((first_c, w1c), (second_c, w2c), (first_u, w1u), (second_u, w2u), (zero, wz))
        )
    ]
    for load in loads:
        load.start()

    barrier = pltpu.get_barrier_semaphore()
    for d in range(1, ways):
        pl.semaphore_signal(
            barrier, inc=1, device_id=(branch, dp, lax.rem(me + d, ways)), device_id_type=MESH
        )
    pl.semaphore_signal(barrier, inc=1, device_id=(1 - branch, dp, me), device_id_type=MESH)

    def ag_copy(unit, d, slot):
        return pltpu.make_async_remote_copy(
            src_ref=gathered.at[unit, slot],
            dst_ref=gathered.at[unit, slot],
            send_sem=ag_send.at[unit, d - 1],
            recv_sem=ag_recv.at[unit, d - 1],
            device_id=(branch, dp, lax.rem(me + d, ways)),
            device_id_type=MESH,
        )

    def rs_copy(unit, d):
        peer = lax.rem(me + d, ways)
        return pltpu.make_async_remote_copy(
            src_ref=sends.at[unit, peer],
            dst_ref=lands.at[unit, d - 1],
            send_sem=rs_send.at[unit, d - 1],
            recv_sem=rs_recv.at[unit, d - 1],
            device_id=(branch, dp, peer),
            device_id_type=MESH,
        )

    def own_hidden(unit):
        if unit == 2:
            return unet_hidden[0]
        half = 1 - branch if unit == 0 else branch
        return control_hidden[0, half, 0]

    for unit in range(3):
        gathered[unit, me] = norm_silu(own_hidden(unit).astype(jnp.float32)).astype(jnp.bfloat16)
        if unit == 0:
            pl.semaphore_wait(barrier, ways)
        for d in range(1, ways):
            ag_copy(unit, d, me).start()

    def block(unit, first_weight, second_weight, total, first_load, second_load):
        for d in range(1, ways):
            ag_copy(unit, d, lax.rem(me + ways - d, ways)).wait_recv()
        if first_load is not None:
            first_load.wait()
        half = 2 if unit == 2 else (1 - branch if unit == 0 else branch)
        inner[...] = jnp.broadcast_to(start[half][:, :1], (width, pixels))

        def first_tap(tap, carry):
            dy = tap // 3 - 1
            dx = lax.rem(tap, 3) - 1
            term = jnp.dot(
                first_weight[tap],
                gathered[unit].reshape(channels, pixels),
                preferred_element_type=jnp.float32,
            )
            moved = pltpu.roll(term, lax.rem(2 * pixels - (SIDE * dy + dx), pixels), 1)
            spot = lax.broadcasted_iota(jnp.int32, (1, pixels), 1)
            row = spot // SIDE + dy
            col = lax.rem(spot, SIDE) + dx
            keep = (row >= 0) & (row < SIDE) & (col >= 0) & (col < SIDE)
            inner[...] += jnp.where(keep, moved, 0.0)
            return carry

        lax.fori_loop(0, 9, first_tap, 0)
        flipped[...] = norm_silu(inner[...]).T
        if second_load is not None:
            second_load.wait()

        def second_tap(tap, carry):
            dy = tap // 3 - 1
            dx = lax.rem(tap, 3) - 1
            moved = pltpu.roll(flipped[...], lax.rem(2 * pixels - (SIDE * dy + dx), pixels), 0)
            spot = lax.broadcasted_iota(jnp.int32, (pixels, 1), 0)
            row = spot // SIDE + dy
            col = lax.rem(spot, SIDE) + dx
            keep = (row >= 0) & (row < SIDE) & (col >= 0) & (col < SIDE)
            operand = jnp.where(keep, moved, 0.0).astype(jnp.bfloat16)
            term = jnp.dot(operand, second_weight[tap], preferred_element_type=jnp.float32)

            @pl.when(tap == 0)
            def _():
                total[...] = term

            @pl.when(tap > 0)
            def _():
                total[...] += term

            return carry

        lax.fori_loop(0, 9, second_tap, 0)

    def scatter(unit, total):
        sends[unit] = total[...].T.astype(jnp.bfloat16).reshape(ways, width, pixels)
        for d in range(1, ways):
            rs_copy(unit, d).start()

    def collect(unit):
        summed = own_hidden(unit).astype(jnp.float32) + sends[unit, me].astype(jnp.float32)
        for d in range(1, ways):
            rs_copy(unit, d).wait_recv()
            summed = summed + lands[unit, d - 1].astype(jnp.float32)
        return summed

    block(0, w1c, w2c, total_c, loads[0], loads[1])
    scatter(0, total_c)
    block(1, w1c, w2c, total_c, None, None)
    scatter(1, total_c)
    block(2, w1u, w2u, total_u, loads[2], loads[3])

    def residual(unit):
        half = 1 - branch if unit == 0 else branch
        copy_out = collect(unit).T.astype(jnp.bfloat16)
        term = jnp.dot(copy_out, wz[...], preferred_element_type=jnp.float32)
        return term * scale[half][:1, :1]

    loads[4].wait()
    swap_out[...] = residual(0).astype(jnp.bfloat16)
    swap = pltpu.make_async_remote_copy(
        src_ref=swap_out,
        dst_ref=swap_in,
        send_sem=swap_send,
        recv_sem=swap_recv,
        device_id=(1 - branch, dp, me),
        device_id_type=MESH,
    )
    swap.start()
    total_u[...] += residual(1)
    swap.wait_recv()
    total_u[...] += swap_in[...].astype(jnp.float32)
    scatter(2, total_u)
    out[0] = collect(2).astype(jnp.bfloat16)
    swap.wait_send()
    for unit in range(3):
        for d in range(1, ways):
            ag_copy(unit, d, me).wait_send()
            rs_copy(unit, d).wait_send()


def shards(
    unet_hidden,
    control_hidden,
    timesteps,
    control_scales,
    unet_time_first,
    unet_time_second,
    unet_proj,
    unet_conv_first,
    unet_conv_second,
    control_time_first,
    control_time_second,
    control_proj,
    control_conv_first,
    control_conv_second,
    zero_conv,
):
    ways = lax.axis_size("mp")
    width, pixels = unet_hidden.shape[1], unet_hidden.shape[2]
    channels = ways * width
    halves = timesteps.shape[0]
    waves = sinusoid(timesteps.reshape(halves)).astype(jnp.bfloat16)
    own_wave = lax.dynamic_slice_in_dim(waves, lax.axis_index("branch"), 1, 0)
    start_u = jnp.dot(
        time_embed(own_wave, unet_time_first, unet_time_second),
        unet_proj,
        preferred_element_type=jnp.float32,
    )
    start_c = jnp.dot(
        time_embed(waves, control_time_first[0], control_time_second[0]),
        control_proj[0],
        preferred_element_type=jnp.float32,
    )
    start = jnp.concatenate([start_c, start_u], axis=0)
    start = jnp.broadcast_to(start[:, :, None], (halves + 1, width, 128))
    scale = control_scales[0].astype(jnp.float32) / 8.0
    scale = jnp.broadcast_to(scale[:, :, None], (halves, 8, 128))
    vmem = pl.BlockSpec(memory_space=pltpu.VMEM)
    hbm = pl.BlockSpec(memory_space=pl.ANY)
    taps = unet_conv_first.shape[0]
    bf16, f32 = jnp.bfloat16, jnp.float32
    conv_shape = (taps, width, channels)
    return pl.pallas_call(
        functools.partial(kernel, ways),
        out_shape=jax.ShapeDtypeStruct((1, width, pixels), bf16),
        in_specs=[vmem] * 4 + [hbm] * 5,
        out_specs=vmem,
        scratch_shapes=[
            pltpu.VMEM(conv_shape, bf16),
            pltpu.VMEM(conv_shape, bf16),
            pltpu.VMEM(conv_shape, bf16),
            pltpu.VMEM(conv_shape, bf16),
            pltpu.VMEM((width, channels), bf16),
            pltpu.VMEM((3, ways, width, pixels), bf16),
            pltpu.VMEM((width, pixels), f32),
            pltpu.VMEM((pixels, width), f32),
            pltpu.VMEM((pixels, channels), f32),
            pltpu.VMEM((pixels, channels), f32),
            pltpu.VMEM((3, ways, width, pixels), bf16),
            pltpu.VMEM((3, ways - 1, width, pixels), bf16),
            pltpu.VMEM((pixels, channels), bf16),
            pltpu.VMEM((pixels, channels), bf16),
            pltpu.SemaphoreType.DMA((5,)),
            pltpu.SemaphoreType.DMA((3, ways - 1)),
            pltpu.SemaphoreType.DMA((3, ways - 1)),
            pltpu.SemaphoreType.DMA((3, ways - 1)),
            pltpu.SemaphoreType.DMA((3, ways - 1)),
            pltpu.SemaphoreType.DMA,
            pltpu.SemaphoreType.DMA,
        ],
        compiler_params=pltpu.CompilerParams(
            collective_id=0, has_side_effects=True, vmem_limit_bytes=60 * 1024 * 1024
        ),
    )(
        unet_hidden,
        control_hidden,
        start,
        scale,
        unet_conv_first,
        unet_conv_second,
        control_conv_first[0],
        control_conv_second[0],
        zero_conv[0],
    )


def solution(mesh):
    in_specs = (
        P(("branch", "dp"), "mp", None),
        P("branch", None, "dp", "mp", None),
        P(None, "dp"),
        P("branch", None, "dp"),
        P(),
        P(),
        P(None, "mp"),
        P(None, "mp", None),
        P(None, "mp", None),
        P("branch", None, None),
        P("branch", None, None),
        P("branch", None, "mp"),
        P("branch", None, "mp", None),
        P("branch", None, "mp", None),
        P("branch", "mp", None),
    )
    out_specs = P(("branch", "dp"), "mp", None)
    return jax.shard_map(shards, mesh=mesh, in_specs=in_specs, out_specs=out_specs, check_vma=False)
```

```python
import functools
import math

import jax
import jax.numpy as jnp
from jax import lax
from jax.experimental import pallas as pl
from jax.experimental.pallas import tpu as pltpu
from jax.sharding import PartitionSpec as P

TDIM = 320
GROUP = 40
SIDE = 16
MESH = pl.DeviceIdType.MESH


def sinusoid(step_ids):
    half_width = TDIM // 2
    frequency = jnp.exp(-math.log(10000.0) * jnp.arange(half_width, dtype=jnp.float32) / half_width)
    angles = step_ids.astype(jnp.float32)[:, None] * frequency[None, :]
    return jnp.concatenate([jnp.cos(angles), jnp.sin(angles)], axis=1)


def norm_silu(values):
    width, pixels = values.shape
    grouped = values.reshape(width // GROUP, GROUP, pixels)
    count = 1.0 / (GROUP * pixels)
    mean = jnp.sum(jnp.sum(grouped, axis=1, keepdims=True), axis=2, keepdims=True) * count
    centered = grouped - mean
    var = jnp.sum(jnp.sum(centered * centered, axis=1, keepdims=True), axis=2, keepdims=True) * count
    normed = centered * lax.rsqrt(var + 1e-05)
    return jax.nn.silu(normed).reshape(width, pixels)


def kernel(
    ways,
    unet_hidden,
    control_hidden,
    waves,
    scale,
    hbm_time_first_c,
    hbm_time_second_c,
    hbm_proj_c,
    hbm_time_first_u,
    hbm_time_second_u,
    hbm_proj_u,
    first_c,
    second_c,
    first_u,
    second_u,
    zero,
    out,
    time_first,
    time_second,
    proj,
    w1c,
    w2c,
    w1u,
    w2u,
    wz,
    gathered,
    start,
    inner,
    flipped,
    total_c,
    total_u,
    sends,
    lands,
    swap_out,
    swap_in,
    load_sem,
    ag_send,
    ag_recv,
    rs_send,
    rs_recv,
    swap_send,
    swap_recv,
):
    branch = lax.axis_index("branch")
    dp = lax.axis_index("dp")
    me = lax.axis_index("mp")
    width, pixels = unet_hidden.shape[1], unet_hidden.shape[2]
    channels = ways * width
    last = ways - 1

    loads = [
        pltpu.make_async_copy(src, dst, load_sem.at[i])
        for i, (src, dst) in enumerate(
            (
                (hbm_time_first_c, time_first.at[0]),
                (hbm_time_second_c, time_second.at[0]),
                (hbm_proj_c, proj.at[0]),
                (hbm_time_first_u, time_first.at[1]),
                (hbm_time_second_u, time_second.at[1]),
                (hbm_proj_u, proj.at[1]),
                (first_c, w1c),
                (second_c, w2c),
                (first_u, w1u),
                (second_u, w2u),
                (zero, wz),
            )
        )
    ]
    for load in loads:
        load.start()

    barrier = pltpu.get_barrier_semaphore()

    def greet(inside, coord):
        @pl.when(inside)
        def _():
            pl.semaphore_signal(barrier, inc=1, device_id=coord, device_id_type=MESH)

    greet(me < last, (branch, dp, me + 1))
    greet(me > 0, (branch, dp, me - 1))
    pl.semaphore_signal(barrier, inc=1, device_id=(1 - branch, dp, me), device_id_type=MESH)

    def wait_barrier():
        edge = (me == 0) | (me == last)

        @pl.when(edge)
        def _():
            pl.semaphore_wait(barrier, 2)

        @pl.when(jnp.logical_not(edge))
        def _():
            pl.semaphore_wait(barrier, 3)

    def ag_copy(unit, side, hop, slot):
        return pltpu.make_async_remote_copy(
            src_ref=gathered.at[unit, slot],
            dst_ref=gathered.at[unit, slot],
            send_sem=ag_send.at[unit, side, hop],
            recv_sem=ag_recv.at[unit, side, hop],
            device_id=(branch, dp, me + 1 - 2 * side),
            device_id_type=MESH,
        )

    def ag_step(unit, hop, waits=True, sends_on=True):
        for side in range(2):
            from_slot = me - hop if side == 0 else me + hop
            here = (from_slot >= 0) & (from_slot <= last)
            onward = here & ((me < last) if side == 0 else (me > 0))

            if waits:

                @pl.when(here)
                def _():
                    ag_copy(unit, side, hop - 1, from_slot).wait_recv()

            if sends_on:

                @pl.when(onward)
                def _():
                    ag_copy(unit, side, hop, from_slot).start()

    def ag_drain(unit):
        for hop in range(last):
            for side in range(2):
                from_slot = me - hop if side == 0 else me + hop
                here = (from_slot >= 0) & (from_slot <= last)
                onward = here & ((me < last) if side == 0 else (me > 0))

                @pl.when(onward)
                def _():
                    ag_copy(unit, side, hop, from_slot).wait_send()

    def rs_copy(unit, side, dest):
        return pltpu.make_async_remote_copy(
            src_ref=sends.at[unit, dest],
            dst_ref=lands.at[unit, side, dest],
            send_sem=rs_send.at[unit, dest],
            recv_sem=rs_recv.at[unit, side, dest],
            device_id=(branch, dp, me + 1 - 2 * side),
            device_id_type=MESH,
        )

    def rs_start(unit):
        @pl.when(me == 0)
        def _():
            for dest in range(last, 0, -1):
                rs_copy(unit, 0, dest).start()

        @pl.when(me == last)
        def _():
            for dest in range(last):
                rs_copy(unit, 1, dest).start()

    def rs_slot(unit, slot):
        for side in range(2):
            place = me if side == 0 else last - me
            dest = last - slot + place if side == 0 else slot - place

            @pl.when((place >= 1) & (place <= slot))
            def _():
                rs_copy(unit, side, dest).wait_recv()
                added = sends[unit, dest].astype(jnp.float32) + lands[unit, side, dest].astype(
                    jnp.float32
                )
                sends[unit, dest] = added.astype(jnp.bfloat16)
                rs_copy(unit, side, dest).start()

    def rs_drain(unit):
        for dest in range(ways):

            @pl.when(dest > me)
            def _():
                rs_copy(unit, 0, dest).wait_send()

            @pl.when(dest < me)
            def _():
                rs_copy(unit, 1, dest).wait_send()

    def own_hidden(unit):
        if unit == 2:
            return unet_hidden[0]
        half = 1 - branch if unit == 0 else branch
        return control_hidden[0, half, 0]

    def prepare(unit):
        gathered[unit, me] = norm_silu(own_hidden(unit).astype(jnp.float32)).astype(jnp.bfloat16)

    def embed(block):
        for load in loads[3 * block : 3 * block + 3]:
            load.wait()
        act = waves[...]
        for weight in (time_first, time_second):
            act = jax.nn.silu(
                jnp.dot(act, weight[block], preferred_element_type=jnp.float32)
            ).astype(jnp.bfloat16)
        start[block] = jnp.dot(act, proj[block], preferred_element_type=jnp.float32).T

    def keep_of(tap, shape, axis):
        dy = tap // 3 - 1
        dx = lax.rem(tap, 3) - 1
        spot = lax.broadcasted_iota(jnp.int32, shape, axis)
        row = spot // SIDE + dy
        col = lax.rem(spot, SIDE) + dx
        keep = (row >= 0) & (row < SIDE) & (col >= 0) & (col < SIDE)
        return keep, lax.rem(2 * pixels - (SIDE * dy + dx), pixels)

    def block(unit, first_weight, second_weight, total, first_load, second_load, hooks):
        ag_step(unit, last, sends_on=False)
        if first_load is not None:
            first_load.wait()
        row = 0 if unit == 0 else 1
        inner[...] = jnp.broadcast_to(start[unit // 2][:, row : row + 1], (width, pixels))

        def run(step):
            for place, hook in hooks:
                pl.when(step == place)(hook)

        def first_tap(tap, carry):
            run(tap)
            term = jnp.dot(
                first_weight[tap],
                gathered[unit].reshape(channels, pixels),
                preferred_element_type=jnp.float32,
            )
            keep, shift = keep_of(tap, (1, pixels), 1)
            inner[...] += jnp.where(keep, pltpu.roll(term, shift, 1), 0.0)
            return carry

        lax.fori_loop(0, 9, first_tap, 0)
        flipped[...] = norm_silu(inner[...]).T
        if second_load is not None:
            second_load.wait()
        total[...] = jnp.zeros_like(total)

        def second_tap(tap, carry):
            run(tap + 9)
            keep, shift = keep_of(tap, (pixels, 1), 0)
            operand = jnp.where(keep, pltpu.roll(flipped[...], shift, 0), 0.0).astype(jnp.bfloat16)
            total[...] += jnp.dot(operand, second_weight[tap], preferred_element_type=jnp.float32)
            return carry

        lax.fori_loop(0, 9, second_tap, 0)

    def scatter(unit, total):
        sends[unit] = total[...].T.astype(jnp.bfloat16).reshape(ways, width, pixels)
        rs_start(unit)

    def collect(unit):
        inner[...] = own_hidden(unit).astype(jnp.float32) + sends[unit, me].astype(jnp.float32)
        for side, inside in ((0, me > 0), (1, me < last)):

            @pl.when(inside)
            def _():
                rs_copy(unit, side, me).wait_recv()
                inner[...] += lands[unit, side, me].astype(jnp.float32)

        return inner[...]

    def residual(unit):
        half = 1 - branch if unit == 0 else branch
        copy_out = collect(unit).T.astype(jnp.bfloat16)
        term = jnp.dot(copy_out, wz[...], preferred_element_type=jnp.float32)
        return term * scale[half][:1, :1]

    def spread(first, span, count):
        return [first + i * span // max(count, 1) for i in range(count)]

    prepare(0)
    wait_barrier()
    ag_step(0, 0, waits=False)
    prepare(1)
    prepare(2)
    relays = range(1, last)
    for hop in relays:
        ag_step(0, hop)
        if hop == 1:
            embed(0)
    ag_step(1, 0, waits=False)
    embed(1)

    def relay_hook(unit, hop):
        def hook():
            ag_step(unit, hop)
            if unit == 1 and hop == last - 1:
                ag_step(2, 0, waits=False)

        return hook

    def slot_hook(unit, slot):
        return lambda: rs_slot(unit, slot)

    block(
        0, w1c, w2c, total_c, loads[6], loads[7],
        [(p, relay_hook(1, h)) for p, h in zip(spread(4, 12, len(relays)), relays)],
    )
    scatter(0, total_c)
    block(
        1, w1c, w2c, total_c, None, None,
        [(p, relay_hook(2, h)) for p, h in zip(spread(1, 12, len(relays)), relays)]
        + [(p, slot_hook(0, k)) for p, k in zip(spread(8, 10, len(relays)), relays)],
    )
    scatter(1, total_c)
    block(
        2, w1u, w2u, total_u, loads[8], loads[9],
        [(p, slot_hook(1, k)) for p, k in zip(spread(6, 12, len(relays)), relays)],
    )
    loads[10].wait()
    swap_out[...] = residual(0).astype(jnp.bfloat16)
    swap = pltpu.make_async_remote_copy(
        src_ref=swap_out,
        dst_ref=swap_in,
        send_sem=swap_send,
        recv_sem=swap_recv,
        device_id=(1 - branch, dp, me),
        device_id_type=MESH,
    )
    swap.start()
    total_u[...] += residual(1)
    swap.wait_recv()
    total_u[...] += swap_in[...].astype(jnp.float32)
    scatter(2, total_u)
    for slot in relays:
        rs_slot(2, slot)
    out[0] = collect(2).astype(jnp.bfloat16)
    swap.wait_send()
    for unit in range(3):
        ag_drain(unit)
        rs_drain(unit)


def shards(
    unet_hidden,
    control_hidden,
    timesteps,
    control_scales,
    unet_time_first,
    unet_time_second,
    unet_proj,
    unet_conv_first,
    unet_conv_second,
    control_time_first,
    control_time_second,
    control_proj,
    control_conv_first,
    control_conv_second,
    zero_conv,
):
    ways = lax.axis_size("mp")
    width, pixels = unet_hidden.shape[1], unet_hidden.shape[2]
    channels = ways * width
    halves = timesteps.shape[0]
    branch = lax.axis_index("branch")
    steps = timesteps.reshape(halves)
    waves = sinusoid(jnp.stack([steps[1 - branch], steps[branch]])).astype(jnp.bfloat16)
    waves = jnp.pad(waves, ((0, 16 - halves), (0, 0)))
    scale = control_scales[0].astype(jnp.float32) / 8.0
    scale = jnp.broadcast_to(scale[:, :, None], (halves, 8, 128))
    vmem = pl.BlockSpec(memory_space=pltpu.VMEM)
    hbm = pl.BlockSpec(memory_space=pl.ANY)
    taps = unet_conv_first.shape[0]
    bf16, f32 = jnp.bfloat16, jnp.float32
    conv_shape = (taps, width, channels)
    return pl.pallas_call(
        functools.partial(kernel, ways),
        out_shape=jax.ShapeDtypeStruct((1, width, pixels), bf16),
        in_specs=[vmem] * 4 + [hbm] * 11,
        out_specs=vmem,
        scratch_shapes=[
            pltpu.VMEM((2,) + unet_time_first.shape, bf16),
            pltpu.VMEM((2,) + unet_time_second.shape, bf16),
            pltpu.VMEM((2,) + unet_proj.shape, bf16),
            pltpu.VMEM(conv_shape, bf16),
            pltpu.VMEM(conv_shape, bf16),
            pltpu.VMEM(conv_shape, bf16),
            pltpu.VMEM(conv_shape, bf16),
            pltpu.VMEM((width, channels), bf16),
            pltpu.VMEM((3, ways, width, pixels), bf16),
            pltpu.VMEM((2, width, 16), f32),
            pltpu.VMEM((width, pixels), f32),
            pltpu.VMEM((pixels, width), f32),
            pltpu.VMEM((pixels, channels), f32),
            pltpu.VMEM((pixels, channels), f32),
            pltpu.VMEM((3, ways, width, pixels), bf16),
            pltpu.VMEM((3, 2, ways, width, pixels), bf16),
            pltpu.VMEM((pixels, channels), bf16),
            pltpu.VMEM((pixels, channels), bf16),
            pltpu.SemaphoreType.DMA((11,)),
            pltpu.SemaphoreType.DMA((3, 2, ways - 1)),
            pltpu.SemaphoreType.DMA((3, 2, ways - 1)),
            pltpu.SemaphoreType.DMA((3, ways)),
            pltpu.SemaphoreType.DMA((3, 2, ways)),
            pltpu.SemaphoreType.DMA,
            pltpu.SemaphoreType.DMA,
        ],
        compiler_params=pltpu.CompilerParams(
            collective_id=0, has_side_effects=True, vmem_limit_bytes=62 * 1024 * 1024
        ),
    )(
        unet_hidden,
        control_hidden,
        waves,
        scale,
        control_time_first[0],
        control_time_second[0],
        control_proj[0],
        unet_time_first,
        unet_time_second,
        unet_proj,
        control_conv_first[0],
        control_conv_second[0],
        unet_conv_first,
        unet_conv_second,
        zero_conv[0],
    )


def solution(mesh):
    in_specs = (
        P(("branch", "dp"), "mp", None),
        P("branch", None, "dp", "mp", None),
        P(None, "dp"),
        P("branch", None, "dp"),
        P(),
        P(),
        P(None, "mp"),
        P(None, "mp", None),
        P(None, "mp", None),
        P("branch", None, None),
        P("branch", None, None),
        P("branch", None, "mp"),
        P("branch", None, "mp", None),
        P("branch", None, "mp", None),
        P("branch", "mp", None),
    )
    out_specs = P(("branch", "dp"), "mp", None)
    return jax.shard_map(shards, mesh=mesh, in_specs=in_specs, out_specs=out_specs, check_vma=False)
```

```python
import functools
import math

import jax
import jax.numpy as jnp
from jax import lax
from jax.experimental import pallas as pl
from jax.experimental.pallas import tpu as pltpu
from jax.sharding import PartitionSpec as P

TDIM = 320
GROUP = 40
PIECES = 2
SIDE = 16
MESH = pl.DeviceIdType.MESH


def sinusoid(step_ids):
    half_width = TDIM // 2
    frequency = jnp.exp(-math.log(10000.0) * jnp.arange(half_width, dtype=jnp.float32) / half_width)
    angles = step_ids.astype(jnp.float32)[:, None] * frequency[None, :]
    return jnp.concatenate([jnp.cos(angles), jnp.sin(angles)], axis=1)


def norm_silu(values):
    width, pixels = values.shape
    grouped = values.reshape(width // GROUP, GROUP, pixels)
    count = 1.0 / (GROUP * pixels)
    mean = jnp.sum(jnp.sum(grouped, axis=1, keepdims=True), axis=2, keepdims=True) * count
    centered = grouped - mean
    var = jnp.sum(jnp.sum(centered * centered, axis=1, keepdims=True), axis=2, keepdims=True) * count
    normed = centered * lax.rsqrt(var + 1e-05)
    return jax.nn.silu(normed).reshape(width, pixels)


def kernel(
    ways,
    unet_hidden,
    control_hidden,
    waves,
    scale,
    hbm_time_first_c,
    hbm_time_second_c,
    hbm_proj_c,
    hbm_time_first_u,
    hbm_time_second_u,
    hbm_proj_u,
    first_c,
    second_c,
    first_u,
    second_u,
    zero,
    out,
    time_first,
    time_second,
    proj,
    w1c,
    w2c,
    w1u,
    w2u,
    wz,
    gathered,
    start,
    inner,
    flipped,
    total_c,
    total_u,
    sends,
    lands,
    swap_out,
    swap_in,
    load_sem,
    ag_send,
    ag_recv,
    rs_send,
    rs_recv,
    swap_send,
    swap_recv,
):
    branch = lax.axis_index("branch")
    dp = lax.axis_index("dp")
    me = lax.axis_index("mp")
    width, pixels = unet_hidden.shape[1], unet_hidden.shape[2]
    channels = ways * width
    last = ways - 1

    loads = [
        pltpu.make_async_copy(src, dst, load_sem.at[i])
        for i, (src, dst) in enumerate(
            (
                (hbm_time_first_c, time_first.at[0]),
                (hbm_time_second_c, time_second.at[0]),
                (hbm_proj_c, proj.at[0]),
                (hbm_time_first_u, time_first.at[1]),
                (hbm_time_second_u, time_second.at[1]),
                (hbm_proj_u, proj.at[1]),
                (first_c, w1c),
                (second_c, w2c),
                (first_u, w1u),
                (second_u, w2u),
                (zero, wz),
            )
        )
    ]
    for load in loads:
        load.start()

    barrier = pltpu.get_barrier_semaphore()

    def greet(inside, coord):
        @pl.when(inside)
        def _():
            pl.semaphore_signal(barrier, inc=1, device_id=coord, device_id_type=MESH)

    greet(me < last, (branch, dp, me + 1))
    greet(me > 0, (branch, dp, me - 1))
    pl.semaphore_signal(barrier, inc=1, device_id=(1 - branch, dp, me), device_id_type=MESH)

    def wait_barrier():
        edge = (me == 0) | (me == last)

        @pl.when(edge)
        def _():
            pl.semaphore_wait(barrier, 2)

        @pl.when(jnp.logical_not(edge))
        def _():
            pl.semaphore_wait(barrier, 3)

    def part(piece):
        return pl.ds(piece * (pixels // PIECES), pixels // PIECES)

    def ag_copy(unit, side, hop, slot, piece):
        return pltpu.make_async_remote_copy(
            src_ref=gathered.at[unit, slot, :, part(piece)],
            dst_ref=gathered.at[unit, slot, :, part(piece)],
            send_sem=ag_send.at[unit, side, hop, piece],
            recv_sem=ag_recv.at[unit, side, hop, piece],
            device_id=(branch, dp, me + 1 - 2 * side),
            device_id_type=MESH,
        )

    def ag_step(unit, hop, waits=True, sends_on=True):
        for piece, side in [(p, d) for p in range(PIECES) for d in range(2)]:
            from_slot = me - hop if side == 0 else me + hop
            here = (from_slot >= 0) & (from_slot <= last)
            onward = here & ((me < last) if side == 0 else (me > 0))

            if waits:

                @pl.when(here)
                def _():
                    ag_copy(unit, side, hop - 1, from_slot, piece).wait_recv()

            if sends_on:

                @pl.when(onward)
                def _():
                    ag_copy(unit, side, hop, from_slot, piece).start()

    def ag_drain(unit):
        for hop in range(last):
            for side in range(2):
                from_slot = me - hop if side == 0 else me + hop
                here = (from_slot >= 0) & (from_slot <= last)
                onward = here & ((me < last) if side == 0 else (me > 0))

                @pl.when(onward)
                def _():
                    for piece in range(PIECES):
                        ag_copy(unit, side, hop, from_slot, piece).wait_send()

    def rs_copy(unit, side, dest, piece):
        return pltpu.make_async_remote_copy(
            src_ref=sends.at[unit, dest, :, part(piece)],
            dst_ref=lands.at[unit, side, dest, :, part(piece)],
            send_sem=rs_send.at[unit, dest, piece],
            recv_sem=rs_recv.at[unit, side, dest, piece],
            device_id=(branch, dp, me + 1 - 2 * side),
            device_id_type=MESH,
        )

    def rs_start(unit):
        @pl.when(me == 0)
        def _():
            for dest in range(last, 0, -1):
                for piece in range(PIECES):
                    rs_copy(unit, 0, dest, piece).start()

        @pl.when(me == last)
        def _():
            for dest in range(last):
                for piece in range(PIECES):
                    rs_copy(unit, 1, dest, piece).start()

    def rs_slot(unit, slot):
        for piece, side in [(p, d) for p in range(PIECES) for d in range(2)]:
            place = me if side == 0 else last - me
            dest = last - slot + place if side == 0 else slot - place

            @pl.when((place >= 1) & (place <= slot))
            def _():
                rs_copy(unit, side, dest, piece).wait_recv()
                added = sends[unit, dest, :, part(piece)].astype(jnp.float32) + lands[
                    unit, side, dest, :, part(piece)
                ].astype(jnp.float32)
                sends[unit, dest, :, part(piece)] = added.astype(jnp.bfloat16)
                rs_copy(unit, side, dest, piece).start()

    def rs_drain(unit):
        for dest in range(ways):

            @pl.when(dest > me)
            def _():
                for piece in range(PIECES):
                    rs_copy(unit, 0, dest, piece).wait_send()

            @pl.when(dest < me)
            def _():
                for piece in range(PIECES):
                    rs_copy(unit, 1, dest, piece).wait_send()

    def own_hidden(unit):
        if unit == 2:
            return unet_hidden[0]
        half = 1 - branch if unit == 0 else branch
        return control_hidden[0, half, 0]

    def prepare(unit):
        gathered[unit, me] = norm_silu(own_hidden(unit).astype(jnp.float32)).astype(jnp.bfloat16)

    def embed(block):
        for load in loads[3 * block : 3 * block + 3]:
            load.wait()
        act = waves[...]
        for weight in (time_first, time_second):
            act = jax.nn.silu(
                jnp.dot(act, weight[block], preferred_element_type=jnp.float32)
            ).astype(jnp.bfloat16)
        start[block] = lax.dot_general(
            proj[block], act, (((1,), (1,)), ((), ())), preferred_element_type=jnp.float32
        )

    def keep_of(tap, shape, axis):
        dy = tap // 3 - 1
        dx = lax.rem(tap, 3) - 1
        spot = lax.broadcasted_iota(jnp.int32, shape, axis)
        row = spot // SIDE + dy
        col = lax.rem(spot, SIDE) + dx
        keep = (row >= 0) & (row < SIDE) & (col >= 0) & (col < SIDE)
        return keep, lax.rem(2 * pixels - (SIDE * dy + dx), pixels)

    def block(unit, first_weight, second_weight, total, first_load, second_load, hooks):
        ag_step(unit, last, sends_on=False)
        if first_load is not None:
            first_load.wait()
        other = branch == 1 if unit == 0 else branch == 0
        columns = start[unit // 2]
        inner[...] = jnp.broadcast_to(
            jnp.where(other, columns[:, :1], columns[:, 1:2]), (width, pixels)
        )

        def run(step):
            for place, hook in hooks:
                pl.when(step == place)(hook)

        def first_tap(tap, carry):
            run(tap)
            term = jnp.dot(
                first_weight[tap],
                gathered[unit].reshape(channels, pixels),
                preferred_element_type=jnp.float32,
            )
            keep, shift = keep_of(tap, (1, pixels), 1)
            inner[...] += jnp.where(keep, pltpu.roll(term, shift, 1), 0.0)
            return carry

        lax.fori_loop(0, 9, first_tap, 0)
        flipped[...] = norm_silu(inner[...]).T
        if second_load is not None:
            second_load.wait()
        total[...] = jnp.zeros_like(total)

        def second_tap(tap, carry):
            run(tap + 9)
            keep, shift = keep_of(tap, (pixels, 1), 0)
            operand = jnp.where(keep, pltpu.roll(flipped[...], shift, 0), 0.0).astype(jnp.bfloat16)
            total[...] += jnp.dot(operand, second_weight[tap], preferred_element_type=jnp.float32)
            return carry

        lax.fori_loop(0, 9, second_tap, 0)

    def scatter(unit, total):
        sends[unit] = total[...].T.astype(jnp.bfloat16).reshape(ways, width, pixels)
        rs_start(unit)

    def collect(unit):
        inner[...] = own_hidden(unit).astype(jnp.float32) + sends[unit, me].astype(jnp.float32)
        for side, inside in ((0, me > 0), (1, me < last)):

            @pl.when(inside)
            def _():
                for piece in range(PIECES):
                    rs_copy(unit, side, me, piece).wait_recv()
                inner[...] += lands[unit, side, me].astype(jnp.float32)

        return inner[...]

    def residual(unit):
        half = 1 - branch if unit == 0 else branch
        copy_out = collect(unit).T.astype(jnp.bfloat16)
        term = jnp.dot(copy_out, wz[...], preferred_element_type=jnp.float32)
        return term * (scale[half, 0].astype(jnp.float32) * 0.125)

    def spread(first, span, count):
        return [first + i * span // max(count, 1) for i in range(count)]

    prepare(0)
    wait_barrier()
    ag_step(0, 0, waits=False)
    prepare(1)
    prepare(2)
    relays = range(1, last)
    for hop in relays:
        ag_step(0, hop)
        if hop == 1:
            embed(0)
    ag_step(1, 0, waits=False)
    embed(1)

    def relay_hook(unit, hop):
        def hook():
            ag_step(unit, hop)
            if unit == 1 and hop == last - 1:
                ag_step(2, 0, waits=False)

        return hook

    def slot_hook(unit, slot):
        return lambda: rs_slot(unit, slot)

    block(
        0, w1c, w2c, total_c, loads[6], loads[7],
        [(p, relay_hook(1, h)) for p, h in zip(spread(4, 12, len(relays)), relays)],
    )
    scatter(0, total_c)
    block(
        1, w1c, w2c, total_c, None, None,
        [(p, relay_hook(2, h)) for p, h in zip(spread(1, 12, len(relays)), relays)]
        + [(p, slot_hook(0, k)) for p, k in zip(spread(8, 10, len(relays)), relays)],
    )
    scatter(1, total_c)
    loads[10].wait()
    swap_out[...] = residual(0).astype(jnp.bfloat16)
    swap = pltpu.make_async_remote_copy(
        src_ref=swap_out,
        dst_ref=swap_in,
        send_sem=swap_send,
        recv_sem=swap_recv,
        device_id=(1 - branch, dp, me),
        device_id_type=MESH,
    )
    swap.start()
    block(
        2, w1u, w2u, total_u, loads[8], loads[9],
        [(p, slot_hook(1, k)) for p, k in zip(spread(6, 12, len(relays)), relays)],
    )
    total_u[...] += residual(1)
    swap.wait_recv()
    total_u[...] += swap_in[...].astype(jnp.float32)
    scatter(2, total_u)
    for slot in relays:
        rs_slot(2, slot)
    out[0] = collect(2).astype(jnp.bfloat16)
    swap.wait_send()
    for unit in range(3):
        ag_drain(unit)
        rs_drain(unit)


def shards(
    unet_hidden,
    control_hidden,
    timesteps,
    control_scales,
    unet_time_first,
    unet_time_second,
    unet_proj,
    unet_conv_first,
    unet_conv_second,
    control_time_first,
    control_time_second,
    control_proj,
    control_conv_first,
    control_conv_second,
    zero_conv,
):
    ways = lax.axis_size("mp")
    width, pixels = unet_hidden.shape[1], unet_hidden.shape[2]
    channels = ways * width
    halves = timesteps.shape[0]
    waves = sinusoid(timesteps.reshape(halves)).astype(jnp.bfloat16)
    waves = jnp.pad(waves, ((0, 16 - halves), (0, 0)))
    scale = control_scales[0]
    vmem = pl.BlockSpec(memory_space=pltpu.VMEM)
    hbm = pl.BlockSpec(memory_space=pl.ANY)
    taps = unet_conv_first.shape[0]
    bf16, f32 = jnp.bfloat16, jnp.float32
    conv_shape = (taps, width, channels)
    return pl.pallas_call(
        functools.partial(kernel, ways),
        out_shape=jax.ShapeDtypeStruct((1, width, pixels), bf16),
        in_specs=[vmem] * 3 + [pl.BlockSpec(memory_space=pltpu.SMEM)] + [hbm] * 11,
        out_specs=vmem,
        scratch_shapes=[
            pltpu.VMEM((2,) + unet_time_first.shape, bf16),
            pltpu.VMEM((2,) + unet_time_second.shape, bf16),
            pltpu.VMEM((2,) + unet_proj.shape[::-1], bf16),
            pltpu.VMEM(conv_shape, bf16),
            pltpu.VMEM(conv_shape, bf16),
            pltpu.VMEM(conv_shape, bf16),
            pltpu.VMEM(conv_shape, bf16),
            pltpu.VMEM((width, channels), bf16),
            pltpu.VMEM((3, ways, width, pixels), bf16),
            pltpu.VMEM((2, width, 16), f32),
            pltpu.VMEM((width, pixels), f32),
            pltpu.VMEM((pixels, width), f32),
            pltpu.VMEM((pixels, channels), f32),
            pltpu.VMEM((pixels, channels), f32),
            pltpu.VMEM((3, ways, width, pixels), bf16),
            pltpu.VMEM((3, 2, ways, width, pixels), bf16),
            pltpu.VMEM((pixels, channels), bf16),
            pltpu.VMEM((pixels, channels), bf16),
            pltpu.SemaphoreType.DMA((11,)),
            pltpu.SemaphoreType.DMA((3, 2, ways - 1, PIECES)),
            pltpu.SemaphoreType.DMA((3, 2, ways - 1, PIECES)),
            pltpu.SemaphoreType.DMA((3, ways, PIECES)),
            pltpu.SemaphoreType.DMA((3, 2, ways, PIECES)),
            pltpu.SemaphoreType.DMA,
            pltpu.SemaphoreType.DMA,
        ],
        compiler_params=pltpu.CompilerParams(
            collective_id=0, has_side_effects=True, vmem_limit_bytes=62 * 1024 * 1024
        ),
    )(
        unet_hidden,
        control_hidden,
        waves,
        scale,
        control_time_first[0],
        control_time_second[0],
        control_proj[0].T,
        unet_time_first,
        unet_time_second,
        unet_proj.T,
        control_conv_first[0],
        control_conv_second[0],
        unet_conv_first,
        unet_conv_second,
        zero_conv[0],
    )


def solution(mesh):
    in_specs = (
        P(("branch", "dp"), "mp", None),
        P("branch", None, "dp", "mp", None),
        P(None, "dp"),
        P("branch", None, "dp"),
        P(),
        P(),
        P(None, "mp"),
        P(None, "mp", None),
        P(None, "mp", None),
        P("branch", None, None),
        P("branch", None, None),
        P("branch", None, "mp"),
        P("branch", None, "mp", None),
        P("branch", None, "mp", None),
        P("branch", "mp", None),
    )
    out_specs = P(("branch", "dp"), "mp", None)
    return jax.shard_map(shards, mesh=mesh, in_specs=in_specs, out_specs=out_specs, check_vma=False)
```

```python
import functools
import math

import jax
import jax.numpy as jnp
from jax import lax
from jax.experimental import pallas as pl
from jax.experimental.pallas import tpu as pltpu
from jax.sharding import PartitionSpec as P

TDIM = 320
GROUP = 40
PIECES = 2
SIDE = 16
MESH = pl.DeviceIdType.MESH


def sinusoid(step_ids):
    half_width = TDIM // 2
    frequency = jnp.exp(-math.log(10000.0) * jnp.arange(half_width, dtype=jnp.float32) / half_width)
    angles = step_ids.astype(jnp.float32)[:, None] * frequency[None, :]
    return jnp.concatenate([jnp.cos(angles), jnp.sin(angles)], axis=1)


def norm_silu(values):
    width, pixels = values.shape
    grouped = values.reshape(width // GROUP, GROUP, pixels)
    count = 1.0 / (GROUP * pixels)
    mean = jnp.sum(jnp.sum(grouped, axis=1, keepdims=True), axis=2, keepdims=True) * count
    centered = grouped - mean
    var = jnp.sum(jnp.sum(centered * centered, axis=1, keepdims=True), axis=2, keepdims=True) * count
    normed = centered * lax.rsqrt(var + 1e-05)
    return jax.nn.silu(normed).reshape(width, pixels)


def kernel(
    ways,
    unet_hidden,
    control_hidden,
    waves,
    scale,
    hbm_time_first_c,
    hbm_time_second_c,
    hbm_proj_c,
    hbm_time_first_u,
    hbm_time_second_u,
    hbm_proj_u,
    first_c,
    second_c,
    first_u,
    second_u,
    zero,
    out,
    time_first,
    time_second,
    proj,
    w1c,
    w2c,
    w1u,
    w2u,
    wz,
    gathered,
    start,
    inner,
    flipped,
    total_c,
    total_u,
    sends,
    lands,
    swap_out,
    swap_in,
    load_sem,
    ag_send,
    ag_recv,
    rs_send,
    rs_recv,
    swap_send,
    swap_recv,
):
    branch = lax.axis_index("branch")
    dp = lax.axis_index("dp")
    me = lax.axis_index("mp")
    width, pixels = unet_hidden.shape[1], unet_hidden.shape[2]
    channels = ways * width
    last = ways - 1

    loads = [
        pltpu.make_async_copy(src, dst, load_sem.at[i])
        for i, (src, dst) in enumerate(
            (
                (hbm_time_first_c, time_first.at[0]),
                (hbm_time_second_c, time_second.at[0]),
                (hbm_proj_c, proj.at[0]),
                (hbm_time_first_u, time_first.at[1]),
                (hbm_time_second_u, time_second.at[1]),
                (hbm_proj_u, proj.at[1]),
                (first_c, w1c),
                (second_c, w2c),
                (first_u, w1u),
                (second_u, w2u),
                (zero, wz),
            )
        )
    ]
    for load in loads:
        load.start()

    barrier = pltpu.get_barrier_semaphore()

    def greet(inside, coord):
        @pl.when(inside)
        def _():
            pl.semaphore_signal(barrier, inc=1, device_id=coord, device_id_type=MESH)

    greet(me < last, (branch, dp, me + 1))
    greet(me > 0, (branch, dp, me - 1))
    pl.semaphore_signal(barrier, inc=1, device_id=(1 - branch, dp, me), device_id_type=MESH)

    def wait_barrier():
        edge = (me == 0) | (me == last)

        @pl.when(edge)
        def _():
            pl.semaphore_wait(barrier, 2)

        @pl.when(jnp.logical_not(edge))
        def _():
            pl.semaphore_wait(barrier, 3)

    def part(piece):
        return pl.ds(piece * (pixels // PIECES), pixels // PIECES)

    def ag_copy(unit, side, hop, slot, piece):
        return pltpu.make_async_remote_copy(
            src_ref=gathered.at[unit, slot, :, part(piece)],
            dst_ref=gathered.at[unit, slot, :, part(piece)],
            send_sem=ag_send.at[unit, side, hop, piece],
            recv_sem=ag_recv.at[unit, side, hop, piece],
            device_id=(branch, dp, me + 1 - 2 * side),
            device_id_type=MESH,
        )

    def ag_step(unit, hop, waits=True, sends_on=True):
        for piece, side in [(p, d) for p in range(PIECES) for d in range(2)]:
            from_slot = me - hop if side == 0 else me + hop
            here = (from_slot >= 0) & (from_slot <= last)
            onward = here & ((me < last) if side == 0 else (me > 0))

            if waits:

                @pl.when(here)
                def _():
                    ag_copy(unit, side, hop - 1, from_slot, piece).wait_recv()

            if sends_on:

                @pl.when(onward)
                def _():
                    ag_copy(unit, side, hop, from_slot, piece).start()

    def ag_drain(unit):
        for hop in range(last):
            for side in range(2):
                from_slot = me - hop if side == 0 else me + hop
                here = (from_slot >= 0) & (from_slot <= last)
                onward = here & ((me < last) if side == 0 else (me > 0))

                @pl.when(onward)
                def _():
                    for piece in range(PIECES):
                        ag_copy(unit, side, hop, from_slot, piece).wait_send()

    def rs_copy(unit, side, dest, piece):
        return pltpu.make_async_remote_copy(
            src_ref=sends.at[unit, dest, :, part(piece)],
            dst_ref=lands.at[unit, side, dest, :, part(piece)],
            send_sem=rs_send.at[unit, dest, piece],
            recv_sem=rs_recv.at[unit, side, dest, piece],
            device_id=(branch, dp, me + 1 - 2 * side),
            device_id_type=MESH,
        )

    def rs_start(unit):
        @pl.when(me == 0)
        def _():
            for dest in range(last, 0, -1):
                for piece in range(PIECES):
                    rs_copy(unit, 0, dest, piece).start()

        @pl.when(me == last)
        def _():
            for dest in range(last):
                for piece in range(PIECES):
                    rs_copy(unit, 1, dest, piece).start()

    def rs_slot(unit, slot):
        for piece, side in [(p, d) for p in range(PIECES) for d in range(2)]:
            place = me if side == 0 else last - me
            dest = last - slot + place if side == 0 else slot - place

            @pl.when((place >= 1) & (place <= slot))
            def _():
                rs_copy(unit, side, dest, piece).wait_recv()
                added = sends[unit, dest, :, part(piece)].astype(jnp.float32) + lands[
                    unit, side, dest, :, part(piece)
                ].astype(jnp.float32)
                sends[unit, dest, :, part(piece)] = added.astype(jnp.bfloat16)
                rs_copy(unit, side, dest, piece).start()

    def rs_drain(unit):
        for dest in range(ways):

            @pl.when(dest > me)
            def _():
                for piece in range(PIECES):
                    rs_copy(unit, 0, dest, piece).wait_send()

            @pl.when(dest < me)
            def _():
                for piece in range(PIECES):
                    rs_copy(unit, 1, dest, piece).wait_send()

    def own_hidden(unit):
        if unit == 2:
            return unet_hidden[0]
        half = 1 - branch if unit == 0 else branch
        return control_hidden[0, half, 0]

    def prepare(unit):
        gathered[unit, me] = norm_silu(own_hidden(unit).astype(jnp.float32)).astype(jnp.bfloat16)

    def embed(block):
        for load in loads[3 * block : 3 * block + 3]:
            load.wait()
        act = waves[...]
        for weight in (time_first, time_second):
            act = jax.nn.silu(
                jnp.dot(act, weight[block], preferred_element_type=jnp.float32)
            ).astype(jnp.bfloat16)
        start[block] = lax.dot_general(
            proj[block], act, (((1,), (1,)), ((), ())), preferred_element_type=jnp.float32
        )

    def keep_of(tap, shape, axis):
        dy = tap // 3 - 1
        dx = lax.rem(tap, 3) - 1
        spot = lax.broadcasted_iota(jnp.int32, shape, axis)
        row = spot // SIDE + dy
        col = lax.rem(spot, SIDE) + dx
        keep = (row >= 0) & (row < SIDE) & (col >= 0) & (col < SIDE)
        return keep, lax.rem(2 * pixels - (SIDE * dy + dx), pixels)

    def block(unit, first_weight, second_weight, total, first_load, second_load, hooks):
        ag_step(unit, last, sends_on=False)
        if first_load is not None:
            first_load.wait()
        other = branch == 1 if unit == 0 else branch == 0
        columns = start[unit // 2]
        inner[...] = jnp.broadcast_to(
            jnp.where(other, columns[:, :1], columns[:, 1:2]), (width, pixels)
        )

        def run(step):
            for place, hook in hooks:
                pl.when(step == place)(hook)

        def first_tap(tap, carry):
            run(tap)
            term = jnp.dot(
                first_weight[tap],
                gathered[unit].reshape(channels, pixels),
                preferred_element_type=jnp.float32,
            )
            keep, shift = keep_of(tap, (1, pixels), 1)
            inner[...] += jnp.where(keep, pltpu.roll(term, shift, 1), 0.0)
            return carry

        lax.fori_loop(0, 9, first_tap, 0)
        flipped[...] = norm_silu(inner[...]).T
        if second_load is not None:
            second_load.wait()
        total[...] = jnp.zeros_like(total)

        def second_line(line, carry):
            operands = []
            for side in range(3):
                tap = 3 * line + side
                run(tap + 9)
                keep, shift = keep_of(tap, (pixels, 1), 0)
                moved = pltpu.roll(flipped[...], shift, 0)
                operands.append(jnp.where(keep, moved, 0.0).astype(jnp.bfloat16))
            total[...] += jnp.dot(
                jnp.concatenate(operands, axis=1),
                second_weight[pl.ds(3 * line, 3)].reshape(3 * width, channels),
                preferred_element_type=jnp.float32,
            )
            return carry

        lax.fori_loop(0, 3, second_line, 0)

    def scatter(unit, total):
        sends[unit] = total[...].T.astype(jnp.bfloat16).reshape(ways, width, pixels)
        rs_start(unit)

    def collect(unit):
        inner[...] = own_hidden(unit).astype(jnp.float32) + sends[unit, me].astype(jnp.float32)
        for side, inside in ((0, me > 0), (1, me < last)):

            @pl.when(inside)
            def _():
                for piece in range(PIECES):
                    rs_copy(unit, side, me, piece).wait_recv()
                inner[...] += lands[unit, side, me].astype(jnp.float32)

        return inner[...]

    def residual(unit):
        half = 1 - branch if unit == 0 else branch
        copy_out = collect(unit).T.astype(jnp.bfloat16)
        term = jnp.dot(copy_out, wz[...], preferred_element_type=jnp.float32)
        return term * (scale[half, 0].astype(jnp.float32) * 0.125)

    def spread(first, span, count):
        return [first + i * span // max(count, 1) for i in range(count)]

    prepare(0)
    wait_barrier()
    ag_step(0, 0, waits=False)
    prepare(1)
    prepare(2)
    relays = range(1, last)
    for hop in relays:
        ag_step(0, hop)
        if hop == 1:
            embed(0)
    ag_step(1, 0, waits=False)
    embed(1)

    def relay_hook(unit, hop):
        def hook():
            ag_step(unit, hop)
            if unit == 1 and hop == last - 1:
                ag_step(2, 0, waits=False)

        return hook

    def slot_hook(unit, slot):
        return lambda: rs_slot(unit, slot)

    block(
        0, w1c, w2c, total_c, loads[6], loads[7],
        [(p, relay_hook(1, h)) for p, h in zip(spread(4, 12, len(relays)), relays)],
    )
    scatter(0, total_c)
    block(
        1, w1c, w2c, total_c, None, None,
        [(p, relay_hook(2, h)) for p, h in zip(spread(1, 12, len(relays)), relays)]
        + [(p, slot_hook(0, k)) for p, k in zip(spread(8, 10, len(relays)), relays)],
    )
    scatter(1, total_c)
    loads[10].wait()
    swap_out[...] = residual(0).astype(jnp.bfloat16)
    swap = pltpu.make_async_remote_copy(
        src_ref=swap_out,
        dst_ref=swap_in,
        send_sem=swap_send,
        recv_sem=swap_recv,
        device_id=(1 - branch, dp, me),
        device_id_type=MESH,
    )
    swap.start()
    block(
        2, w1u, w2u, total_u, loads[8], loads[9],
        [(p, slot_hook(1, k)) for p, k in zip(spread(6, 12, len(relays)), relays)],
    )
    total_u[...] += residual(1)
    swap.wait_recv()
    total_u[...] += swap_in[...].astype(jnp.float32)
    scatter(2, total_u)
    for slot in relays:
        rs_slot(2, slot)
    out[0] = collect(2).astype(jnp.bfloat16)
    swap.wait_send()
    for unit in range(3):
        ag_drain(unit)
        rs_drain(unit)


def shards(
    unet_hidden,
    control_hidden,
    timesteps,
    control_scales,
    unet_time_first,
    unet_time_second,
    unet_proj,
    unet_conv_first,
    unet_conv_second,
    control_time_first,
    control_time_second,
    control_proj,
    control_conv_first,
    control_conv_second,
    zero_conv,
):
    ways = lax.axis_size("mp")
    width, pixels = unet_hidden.shape[1], unet_hidden.shape[2]
    channels = ways * width
    halves = timesteps.shape[0]
    waves = sinusoid(timesteps.reshape(halves)).astype(jnp.bfloat16)
    waves = jnp.pad(waves, ((0, 16 - halves), (0, 0)))
    scale = control_scales[0]
    vmem = pl.BlockSpec(memory_space=pltpu.VMEM)
    hbm = pl.BlockSpec(memory_space=pl.ANY)
    taps = unet_conv_first.shape[0]
    bf16, f32 = jnp.bfloat16, jnp.float32
    conv_shape = (taps, width, channels)
    return pl.pallas_call(
        functools.partial(kernel, ways),
        out_shape=jax.ShapeDtypeStruct((1, width, pixels), bf16),
        in_specs=[vmem] * 3 + [pl.BlockSpec(memory_space=pltpu.SMEM)] + [hbm] * 11,
        out_specs=vmem,
        scratch_shapes=[
            pltpu.VMEM((2,) + unet_time_first.shape, bf16),
            pltpu.VMEM((2,) + unet_time_second.shape, bf16),
            pltpu.VMEM((2,) + unet_proj.shape[::-1], bf16),
            pltpu.VMEM(conv_shape, bf16),
            pltpu.VMEM(conv_shape, bf16),
            pltpu.VMEM(conv_shape, bf16),
            pltpu.VMEM(conv_shape, bf16),
            pltpu.VMEM((width, channels), bf16),
            pltpu.VMEM((3, ways, width, pixels), bf16),
            pltpu.VMEM((2, width, 16), f32),
            pltpu.VMEM((width, pixels), f32),
            pltpu.VMEM((pixels, width), f32),
            pltpu.VMEM((pixels, channels), f32),
            pltpu.VMEM((pixels, channels), f32),
            pltpu.VMEM((3, ways, width, pixels), bf16),
            pltpu.VMEM((3, 2, ways, width, pixels), bf16),
            pltpu.VMEM((pixels, channels), bf16),
            pltpu.VMEM((pixels, channels), bf16),
            pltpu.SemaphoreType.DMA((11,)),
            pltpu.SemaphoreType.DMA((3, 2, ways - 1, PIECES)),
            pltpu.SemaphoreType.DMA((3, 2, ways - 1, PIECES)),
            pltpu.SemaphoreType.DMA((3, ways, PIECES)),
            pltpu.SemaphoreType.DMA((3, 2, ways, PIECES)),
            pltpu.SemaphoreType.DMA,
            pltpu.SemaphoreType.DMA,
        ],
        compiler_params=pltpu.CompilerParams(
            collective_id=0, has_side_effects=True, vmem_limit_bytes=62 * 1024 * 1024
        ),
    )(
        unet_hidden,
        control_hidden,
        waves,
        scale,
        control_time_first[0],
        control_time_second[0],
        control_proj[0].T,
        unet_time_first,
        unet_time_second,
        unet_proj.T,
        control_conv_first[0],
        control_conv_second[0],
        unet_conv_first,
        unet_conv_second,
        zero_conv[0],
    )


def solution(mesh):
    in_specs = (
        P(("branch", "dp"), "mp", None),
        P("branch", None, "dp", "mp", None),
        P(None, "dp"),
        P("branch", None, "dp"),
        P(),
        P(),
        P(None, "mp"),
        P(None, "mp", None),
        P(None, "mp", None),
        P("branch", None, None),
        P("branch", None, None),
        P("branch", None, "mp"),
        P("branch", None, "mp", None),
        P("branch", None, "mp", None),
        P("branch", "mp", None),
    )
    out_specs = P(("branch", "dp"), "mp", None)
    return jax.shard_map(shards, mesh=mesh, in_specs=in_specs, out_specs=out_specs, check_vma=False)
```
